32 devices in a mesh: sub: 2 (over y), row: 4 (over x, core), col: 4 (over z).
Axes of the slice: x: 2, y: 2, z: 4, core: 2. Of those that a mesh axis runs over, the one named last changes fastest.
Arguments:
- visibility: bfloat16 [2, 16, 512, 4096], P(None, 'sub', 'row', 'col'), may hold values from -13 to 13
- sky_model: bfloat16 [2, 16, 512, 4096], P(None, 'sub', 'row', 'col'), may hold values from -4 to 4, as said below
- antenna_flags: int32 [2, 512], P('sub'), may hold values 0 or 1
- gains_init: float32 [2, 16, 512], P(None, 'sub'), may hold values from -0.5 to 1.5
Outputs:
- gains: float32 [2, 16, 512], P(None, 'sub')
The draws below stay inside these ranges and needn't reach their ends.
Inputs may be any that keep to these rules, and one draw needn't show every extreme that they name: `sky_model`: model visibility parts lie between -4 and 4.
All inputs are finite; a program needn't handle non-finite values.
Results may differ from the reference program's by a relative error of at most 0.0003.
Values sent between devices are 32-bit elements.
A program may use at most 64 MiB of HBM per device.

```python
import jax
import jax.numpy as jnp
from jax import lax

ANTENNAS = 512
CH_SUB = 8
TIMES = 8
ITERS = 3
SUBBANDS = 2
CHANNELS = 16
N_SUB = 2


def sky_draw(key):
    full_shape = (CHANNELS, ANTENNAS, ANTENNAS, TIMES)
    model_re = jnp.clip(jax.random.normal(jax.random.fold_in(key, 11), full_shape, jnp.float32), -4.0, 4.0)
    model_im = jnp.clip(jax.random.normal(jax.random.fold_in(key, 21), full_shape, jnp.float32), -4.0, 4.0)
    base_re = jax.random.uniform(jax.random.fold_in(key, 12), (SUBBANDS, 1, ANTENNAS), jnp.float32, 0.6, 1.3)
    base_im = jax.random.uniform(jax.random.fold_in(key, 22), (SUBBANDS, 1, ANTENNAS), jnp.float32, -0.3, 0.3)
    wiggle = jax.random.uniform(jax.random.fold_in(key, 13), (SUBBANDS, CH_SUB, ANTENNAS), jnp.float32, -0.1, 0.1)
    gain_re = (base_re + wiggle).reshape(CHANNELS, ANTENNAS)
    gain_im = jnp.broadcast_to(base_im, (SUBBANDS, CH_SUB, ANTENNAS)).reshape(CHANNELS, ANTENNAS)
    pair_re = gain_re[:, :, None, None] * gain_re[:, None, :, None] + gain_im[:, :, None, None] * gain_im[:, None, :, None]
    pair_im = gain_im[:, :, None, None] * gain_re[:, None, :, None] - gain_re[:, :, None, None] * gain_im[:, None, :, None]
    noise_re = 0.2 * jnp.clip(jax.random.normal(jax.random.fold_in(key, 14), full_shape, jnp.float32), -4.0, 4.0)
    noise_im = 0.2 * jnp.clip(jax.random.normal(jax.random.fold_in(key, 24), full_shape, jnp.float32), -4.0, 4.0)
    observed_re = pair_re * model_re - pair_im * model_im + noise_re
    observed_im = pair_re * model_im + pair_im * model_re + noise_im
    flat_shape = (CHANNELS, ANTENNAS, ANTENNAS * TIMES)
    model_both = jnp.stack([model_re.reshape(flat_shape), model_im.reshape(flat_shape)], axis=0)
    observed_both = jnp.stack([observed_re.reshape(flat_shape), observed_im.reshape(flat_shape)], axis=0)
    return (model_both, observed_both)


def draw_visibility(key, part):
    return sky_draw(key)[1].astype(jnp.bfloat16)


def draw_sky_model(key, part):
    return sky_draw(key)[0].astype(jnp.bfloat16)


def plant(entries, key, low, high):
    index_at = [jax.random.randint(jax.random.fold_in(key, axis), (), 0, length) for axis, length in enumerate(entries.shape)]
    main_axis = entries.shape.index(max(entries.shape))
    neighbour = index_at[:main_axis] + [(index_at[main_axis] + 1) % entries.shape[main_axis]] + index_at[main_axis + 1:]
    return entries.at[tuple(index_at)].set(low).at[tuple(neighbour)].set(high)


def block_scale(own_key, extent, shards, smallest, top_value):
    level, own = 1.0, jax.random.fold_in(own_key, 6)
    for dim, shards_of in shards:
        draws = jnp.exp(jax.random.uniform(jax.random.fold_in(own, dim), (shards_of,), jnp.float32, smallest / len(shards), top_value / len(shards)))
        level = level * jnp.repeat(draws, extent[dim] // shards_of).reshape([-1 if axis == dim else 1 for axis in range(len(extent))])
    return level


def setup_inputs(seed: int = 0) -> dict:
    splits = jax.random.split(jax.random.key(seed), 5)
    return {
        "visibility": draw_visibility(jax.random.fold_in(splits[4], 71), 0),
        "sky_model": draw_sky_model(jax.random.fold_in(splits[4], 71), 0),
        "antenna_flags": plant((jax.random.randint(splits[2], (SUBBANDS, ANTENNAS), 0, 8) < 7).astype(jnp.int32), jax.random.fold_in(splits[2], 1), 0, 1),
        "gains_init": jnp.clip(-0.5 + 2.0 * jax.random.uniform(splits[3], (2, CHANNELS, ANTENNAS), jnp.float32) ** block_scale(splits[3], (2, CHANNELS, ANTENNAS), ((1, 2),), -0.2, 0.2), -0.5, 1.5),
    }


def reference(visibility, sky_model, antenna_flags, gains_init):
    flag_values = antenna_flags.astype(jnp.float32)
    chan_flags = jnp.repeat(flag_values, CH_SUB, axis=0)
    off_diagonal = jnp.float32(1.0) - jnp.eye(ANTENNAS, dtype=jnp.float32)

    def prepare(bundle):
        vis_real, vis_imag, model_real, model_imag, flag_slice = bundle
        shape_three = (ANTENNAS, ANTENNAS, TIMES)
        vis_re = vis_real.astype(jnp.float32).reshape(shape_three)
        vis_im = vis_imag.astype(jnp.float32).reshape(shape_three)
        mod_re = model_real.astype(jnp.float32).reshape(shape_three)
        mod_im = model_imag.astype(jnp.float32).reshape(shape_three)
        weight = flag_slice[:, None] * flag_slice[None, :] * off_diagonal
        cross_re = jnp.sum(vis_re * mod_re + vis_im * mod_im, axis=2) * weight
        cross_im = jnp.sum(vis_im * mod_re - vis_re * mod_im, axis=2) * weight
        power_sum = jnp.sum(mod_re * mod_re + mod_im * mod_im, axis=2) * weight
        return cross_re, cross_im, power_sum

    cross_re, cross_im, power_sum = lax.map(prepare, (visibility[0], visibility[1], sky_model[0], sky_model[1], chan_flags))

    def contract(matrix, vector):
        return jnp.einsum("cpq,cq->cp", matrix, vector, precision=lax.Precision.HIGHEST)

    gain_values = gains_init
    for step_index in range(ITERS):
        gain_re = gain_values[0]
        gain_im = gain_values[1]
        num_re = contract(cross_re, gain_re) - contract(cross_im, gain_im)
        num_im = contract(cross_re, gain_im) + contract(cross_im, gain_re)
        denominator = contract(power_sum, gain_re * gain_re + gain_im * gain_im) + 1.0
        quotient = jnp.stack([num_re / denominator, num_im / denominator], axis=0)
        updated = 0.5 * (quotient + gain_values)
        grouped = updated.reshape(2, N_SUB, CH_SUB, ANTENNAS)
        chan_mean = jnp.mean(grouped, axis=2)
        overall = jnp.mean(chan_mean, axis=1)
        gain_values = (grouped + 0.5 * (overall[:, None, None, :] - chan_mean[:, :, None, :])).reshape(2, CHANNELS, ANTENNAS)
    return gain_values
```

```python
import functools

import jax
import jax.numpy as jnp
from jax import lax
from jax.experimental import pallas as pl
from jax.experimental.pallas import tpu as pltpu
from jax.sharding import PartitionSpec as P

TIMES = 8
ITERS = 3
MESH = pl.DeviceIdType.MESH


def pick_block(value, index, count, width):
    picked = value[..., :width]
    for block in range(1, count):
        picked = jnp.where(index == block, value[..., block * width : (block + 1) * width], picked)
    return picked


def kernel(
    n_sub,
    n_row,
    n_col,
    vis_hbm,
    sky_hbm,
    flags_hbm,
    gains_hbm,
    out_ref,
    vis,
    sky,
    flags,
    gains,
    mats,
    own_gains,
    part_buf,
    prev_buf,
    upd_buf,
    mean_buf,
    last_upd,
    last_mean,
    load_sem,
    part_send,
    part_recv,
    prev_send,
    prev_recv,
    upd_send,
    upd_recv,
    mean_send,
    mean_recv,
    last_upd_send,
    last_upd_recv,
    last_mean_send,
    last_mean_recv,
):
    sub = lax.axis_index("sub")
    row = lax.axis_index("row")
    col = lax.axis_index("col")
    chans, block_rows, wide = vis.shape[1:]
    block_cols = wide // TIMES

    def load_vis(c):
        return pltpu.make_async_copy(vis_hbm.at[:, c], vis.at[:, c], load_sem.at[0, c])

    def load_sky(c):
        return pltpu.make_async_copy(sky_hbm.at[:, c], sky.at[:, c], load_sem.at[1, c])

    load_flags = pltpu.make_async_copy(flags_hbm, flags, load_sem.at[0, chans])
    load_gains = pltpu.make_async_copy(gains_hbm, gains, load_sem.at[1, chans])
    for c in range(chans):
        load_vis(c).start()
        load_sky(c).start()
    load_flags.start()
    load_gains.start()

    barrier = pltpu.get_barrier_semaphore()
    for step in range(1, n_col):
        pl.semaphore_signal(
            barrier, inc=1, device_id=(sub, row, lax.rem(col + step, n_col)), device_id_type=MESH
        )
    for sub_step in range(n_sub):
        for row_step in range(n_row):
            if sub_step or row_step:
                other = (lax.rem(sub + sub_step, n_sub), lax.rem(row + row_step, n_row), col)
                pl.semaphore_signal(barrier, inc=1, device_id=other, device_id_type=MESH)

    tile = min(256, wide)
    tile_cols = tile // TIMES
    selector = (
        lax.broadcasted_iota(jnp.int32, (tile_cols, tile), 1) // TIMES
        == lax.broadcasted_iota(jnp.int32, (tile_cols, tile), 0)
    ).astype(jnp.bfloat16)
    row_ids = row * block_rows + lax.broadcasted_iota(jnp.int32, (tile_cols, block_rows), 1)
    col_ids = col * block_cols + lax.broadcasted_iota(jnp.int32, (tile_cols, block_rows), 0)

    def time_total(values):
        high = values.astype(jnp.bfloat16)
        low = (values - high.astype(jnp.float32)).astype(jnp.bfloat16)
        dims = (((1,), (1,)), ((), ()))
        return lax.dot_general(
            selector, high, dims, preferred_element_type=jnp.float32
        ) + lax.dot_general(selector, low, dims, preferred_element_type=jnp.float32)

    def prepare(c, carry):
        load_vis(c).wait()
        load_sky(c).wait()
        for j in range(wide // tile):
            at = slice(j * tile, (j + 1) * tile)
            vis_re = vis[0, c, :, at].astype(jnp.float32)
            vis_im = vis[1, c, :, at].astype(jnp.float32)
            mod_re = sky[0, c, :, at].astype(jnp.float32)
            mod_im = sky[1, c, :, at].astype(jnp.float32)
            off_diagonal = row_ids != col_ids + j * tile_cols
            to = slice(j * tile_cols, (j + 1) * tile_cols)
            cross_re = time_total(vis_re * mod_re + vis_im * mod_im)
            mats[0, c, to, :] = jnp.where(off_diagonal, cross_re, 0.0)
            cross_im = time_total(vis_im * mod_re - vis_re * mod_im)
            mats[1, c, to, :] = jnp.where(off_diagonal, cross_im, 0.0)
            power = time_total(mod_re * mod_re + mod_im * mod_im)
            mats[2, c, to, :] = jnp.where(off_diagonal, power, 0.0)
        return carry

    lax.fori_loop(0, chans, prepare, 0)

    load_flags.wait()
    load_gains.wait()
    flag_value = flags[...].astype(jnp.float32)
    row_flag = pick_block(flag_value, row, n_row, block_rows)
    col_flag = pick_block(flag_value, col, n_col, block_cols)

    def partial_sums(step, gain_re, gain_im):
        gain_re = (gain_re * col_flag).T
        gain_im = (gain_im * col_flag).T
        for c in range(chans):
            one_re = gain_re[:, c : c + 1]
            one_im = gain_im[:, c : c + 1]
            cross_re, cross_im, power = mats[0, c], mats[1, c], mats[2, c]
            at = (step, col)
            part_buf[(*at, 0, pl.ds(c, 1))] = jnp.sum(
                cross_re * one_re - cross_im * one_im, axis=0, keepdims=True
            )
            part_buf[(*at, 1, pl.ds(c, 1))] = jnp.sum(
                cross_re * one_im + cross_im * one_re, axis=0, keepdims=True
            )
            part_buf[(*at, 2, pl.ds(c, 1))] = jnp.sum(
                power * (one_re * one_re + one_im * one_im), axis=0, keepdims=True
            )

    def send_part(step, source, target, index):
        return pltpu.make_async_remote_copy(
            src_ref=part_buf.at[step, source],
            dst_ref=part_buf.at[step, source],
            send_sem=part_send.at[step, index],
            recv_sem=part_recv.at[step, source],
            device_id=(sub, row, target),
            device_id_type=MESH,
        )

    def send_prev(target, index):
        return pltpu.make_async_remote_copy(
            src_ref=prev_buf,
            dst_ref=prev_buf,
            send_sem=prev_send.at[index],
            recv_sem=prev_recv,
            device_id=(sub, row, target),
            device_id_type=MESH,
        )

    def send_upd(step, target, index):
        return pltpu.make_async_remote_copy(
            src_ref=upd_buf.at[step],
            dst_ref=upd_buf.at[step],
            send_sem=upd_send.at[step, index],
            recv_sem=upd_recv.at[step],
            device_id=(sub, target, col),
            device_id_type=MESH,
        )

    def send_mean(step, source, target, index):
        return pltpu.make_async_remote_copy(
            src_ref=mean_buf.at[step, source],
            dst_ref=mean_buf.at[step, source],
            send_sem=mean_send.at[(step, *index)],
            recv_sem=mean_recv.at[step, source],
            device_id=(*target, col),
            device_id_type=MESH,
        )

    def send_last_upd(source, target, index):
        return pltpu.make_async_remote_copy(
            src_ref=last_upd.at[source],
            dst_ref=last_upd.at[source],
            send_sem=last_upd_send.at[index],
            recv_sem=last_upd_recv.at[source],
            device_id=(sub, target, col),
            device_id_type=MESH,
        )

    def send_last_mean(source, target, index):
        return pltpu.make_async_remote_copy(
            src_ref=last_mean.at[source[0], source[1]],
            dst_ref=last_mean.at[source[0], source[1]],
            send_sem=last_mean_send.at[index[0], index[1]],
            recv_sem=last_mean_recv.at[source[0], source[1]],
            device_id=(*target, col),
            device_id_type=MESH,
        )

    def others(me, count):
        return [(step, lax.rem(me + step, count)) for step in range(1, count)]

    def everyone(me, count):
        return [(step, lax.rem(me + step, count)) for step in range(count)]

    def update(step, previous):
        total = part_buf[step, 0]
        for source in range(1, n_col):
            total = total + part_buf[step, source]
        denominator = total[2] * row_flag + 1.0
        upd_re = 0.5 * (total[0] * row_flag / denominator + previous[0])
        upd_im = 0.5 * (total[1] * row_flag / denominator + previous[1])
        return upd_re, upd_im

    def chan_mean(value):
        return jnp.sum(value, axis=0, keepdims=True) / chans

    home = row == col
    gain_re = pick_block(gains[0], col, n_col, block_cols)
    gain_im = pick_block(gains[1], col, n_col, block_cols)

    for step in range(ITERS):
        last = step == ITERS - 1
        if last:
            @pl.when(home)
            def _():
                prev_buf[0] = gain_re
                prev_buf[1] = gain_im
                for index, target in others(col, n_col):
                    send_prev(target, index).start()

        partial_sums(step, gain_re, gain_im)
        if step == 0:
            pl.semaphore_wait(barrier, n_col - 1 + n_sub * n_row - 1)

        if not last:
            own_gains[0] = gain_re
            own_gains[1] = gain_im

            @pl.when(jnp.logical_not(home))
            def _():
                send_part(step, col, row, 0).start()
                send_upd(step, row, 0).wait_recv()

            @pl.when(home)
            def _():
                for index, source in others(col, n_col):
                    send_part(step, source, col, 0).wait_recv()
                upd_re, upd_im = update(step, own_gains)
                mean_buf[step, sub, 0] = chan_mean(upd_re)
                mean_buf[step, sub, 1] = chan_mean(upd_im)
                upd_buf[step, 0] = upd_re
                upd_buf[step, 1] = upd_im
                for sub_index, sub_target in others(sub, n_sub):
                    for row_index, row_target in everyone(row, n_row):
                        send_mean(step, sub, (sub_target, row_target), (sub_index, row_index)).start()
                for index, target in others(row, n_row):
                    send_upd(step, target, index).start()

            upd_re = upd_buf[step, 0]
            upd_im = upd_buf[step, 1]
            mean_re = chan_mean(upd_re)
            mean_im = chan_mean(upd_im)

            @pl.when(jnp.logical_not(home))
            def _():
                mean_buf[step, sub, 0] = mean_re
                mean_buf[step, sub, 1] = mean_im

            for index, source in others(sub, n_sub):
                send_mean(step, source, (sub, row), (0, 0)).wait_recv()
            overall = mean_buf[step, 0]
            for source in range(1, n_sub):
                overall = overall + mean_buf[step, source]
            overall = overall / n_sub
            gain_re = upd_re + 0.5 * (overall[0] - mean_re)
            gain_im = upd_im + 0.5 * (overall[1] - mean_im)
        else:
            for index, target in others(col, n_col):
                send_part(step, col, target, index).start()

            @pl.when(jnp.logical_not(home))
            def _():
                send_prev(col, 0).wait_recv()

            for index, source in others(col, n_col):
                send_part(step, source, col, 0).wait_recv()
            upd_re, upd_im = update(step, prev_buf)
            last_mean[sub, row, 0] = chan_mean(upd_re)
            last_mean[sub, row, 1] = chan_mean(upd_im)
            last_upd[row, 0] = upd_re
            last_upd[row, 1] = upd_im
            for sub_index, sub_target in others(sub, n_sub):
                for row_index, row_target in everyone(row, n_row):
                    send_last_mean(
                        (sub, row), (sub_target, row_target), (sub_index, row_index)
                    ).start()
            for index, target in others(row, n_row):
                send_last_upd(row, target, index).start()
            for index, source in others(row, n_row):
                send_last_upd(source, row, 0).wait_recv()
                last_mean[sub, source, 0] = chan_mean(last_upd[source, 0])
                last_mean[sub, source, 1] = chan_mean(last_upd[source, 1])
            for sub_index, sub_source in others(sub, n_sub):
                for row_index, row_source in everyone(row, n_row):
                    send_last_mean((sub_source, row_source), (sub, row), (0, 0)).wait_recv()
            for block in range(n_row):
                overall = last_mean[0, block]
                for source in range(1, n_sub):
                    overall = overall + last_mean[source, block]
                overall = overall / n_sub
                shift = 0.5 * (overall - last_mean[sub, block])
                at = slice(block * block_rows, (block + 1) * block_rows)
                out_ref[0, :, at] = last_upd[block, 0] + shift[0]
                out_ref[1, :, at] = last_upd[block, 1] + shift[1]

    for step in range(ITERS - 1):
        @pl.when(jnp.logical_not(home))
        def _():
            send_part(step, col, row, 0).wait_send()

        @pl.when(home)
        def _():
            for sub_index, sub_target in others(sub, n_sub):
                for row_index, row_target in everyone(row, n_row):
                    send_mean(
                        step, sub, (sub_target, row_target), (sub_index, row_index)
                    ).wait_send()
            for index, target in others(row, n_row):
                send_upd(step, target, index).wait_send()

    @pl.when(home)
    def _():
        for index, target in others(col, n_col):
            send_prev(target, index).wait_send()

    for index, target in others(col, n_col):
        send_part(ITERS - 1, col, target, index).wait_send()
    for sub_index, sub_target in others(sub, n_sub):
        for row_index, row_target in everyone(row, n_row):
            send_last_mean(
                (sub, row), (sub_target, row_target), (sub_index, row_index)
            ).wait_send()
    for index, target in others(row, n_row):
        send_last_upd(row, target, index).wait_send()


def body(n_sub, n_row, n_col, visibility, sky_model, antenna_flags, gains_init):
    chans, block_rows, wide = visibility.shape[1:]
    block_cols = wide // TIMES
    assert n_row == n_col and block_rows == block_cols
    dma = pltpu.SemaphoreType.DMA
    part = (chans, block_rows)
    mean = (2, 1, block_rows)
    return pl.pallas_call(
        functools.partial(kernel, n_sub, n_row, n_col),
        out_shape=jax.ShapeDtypeStruct(gains_init.shape, jnp.float32),
        in_specs=[pl.BlockSpec(memory_space=pl.ANY)] * 4,
        out_specs=pl.BlockSpec(memory_space=pltpu.VMEM),
        scratch_shapes=[
            pltpu.VMEM(visibility.shape, visibility.dtype),
            pltpu.VMEM(sky_model.shape, sky_model.dtype),
            pltpu.VMEM(antenna_flags.shape, antenna_flags.dtype),
            pltpu.VMEM(gains_init.shape, jnp.float32),
            pltpu.VMEM((3, chans, block_cols, block_rows), jnp.float32),
            pltpu.VMEM((2, *part), jnp.float32),
            pltpu.VMEM((ITERS, n_col, 3, *part), jnp.float32),
            pltpu.VMEM((2, *part), jnp.float32),
            pltpu.VMEM((ITERS - 1, 2, *part), jnp.float32),
            pltpu.VMEM((ITERS - 1, n_sub, *mean), jnp.float32),
            pltpu.VMEM((n_row, 2, *part), jnp.float32),
            pltpu.VMEM((n_sub, n_row, *mean), jnp.float32),
            dma((2, chans + 1)),
            dma((ITERS, n_col)),
            dma((ITERS, n_col)),
            dma((n_col,)),
            dma(()),
            dma((ITERS - 1, n_row)),
            dma((ITERS - 1,)),
            dma((ITERS - 1, n_sub, n_row)),
            dma((ITERS - 1, n_sub)),
            dma((n_row,)),
            dma((n_row,)),
            dma((n_sub, n_row)),
            dma((n_sub, n_row)),
        ],
        compiler_params=pltpu.CompilerParams(
            collective_id=0, has_side_effects=True, vmem_limit_bytes=67_000_000
        ),
    )(visibility, sky_model, antenna_flags, gains_init)


def solution(mesh):
    return jax.shard_map(
        functools.partial(body, mesh.shape["sub"], mesh.shape["row"], mesh.shape["col"]),
        mesh=mesh,
        in_specs=(
            P(None, "sub", "row", "col"),
            P(None, "sub", "row", "col"),
            P("sub", None),
            P(None, "sub", None),
        ),
        out_specs=P(None, "sub", None),
        check_vma=False,
    )
```
